32 devices in a mesh: groups: 2 (over y), rows: 4 (over z), cols: 4 (over x, core).
Axes of the slice: x: 2, y: 2, z: 4, core: 2. Of those that a mesh axis runs over, the one named last changes fastest.
Arguments:
- tile_blocks: float32 [32, 32, 4, 128, 128], P(('groups', 'rows'), 'cols'), parts along dimension 0, may hold values from -1 to 3
- tile_codes: int32 [32, 32, 3], P(('groups', 'rows'), 'cols'), parts along dimension 0, may hold values from 0 to 3, as said below
- shifts: float32 [16], P('groups'), parts along dimension 0, may hold values from 1.2 to 2.8
- shift_order: int32 [16], P('groups'), parts along dimension 0, may hold values from 0 to 7, each once
- earlier: float32 [16, 32, 32, 128], P(None, ('groups', 'rows'), 'cols'), parts along dimension 1, may hold values from -60 to 60
- start_weights: float32 [32], P('groups'), parts along dimension 0, may hold values from -1 to 1
Outputs:
- new_basis: float32 [8, 32, 32, 128], P(None, ('groups', 'rows'), 'cols'), parts along dimension 1
- upper_factor: float32 [16, 8], P('groups'), parts along dimension 0
- projections: float32 [32, 8], P('groups'), parts along dimension 0
The draws below stay inside these ranges and needn't reach their ends.
There are 2 independent parts, one for each index of `groups`. The reference program is written for one: setup_inputs(seed, part) draws one part's arguments, and reference() takes and returns one part's arrays. A program takes and returns all parts, laid end to end along the dimension named above; each array names one. Nothing has to cross between parts.
Inputs may be any that keep to these rules, and one draw needn't show every extreme that they name: `tile_codes`: the three codes of one block are distinct. `shift_order`: each of 0 to 7 appears once.
All inputs are finite; a program needn't handle non-finite values.
Results may differ from the reference program's by a relative error of at most 0.0003.
Values sent between devices are 32-bit elements; how exact they have to be, the bound alone decides.
A program may use at most 64 MiB of HBM per device.

```python
import math
import jax
import jax.numpy as jnp
from jax import lax

TILE = 128
BASIS = 8
PREV = 16
NBR = 16
NBC = 32


def draw_tile_blocks(key, part):
    key_list = jax.random.split(jax.random.fold_in(key, 11), 2)
    shape_full = (NBR, NBC, 4, TILE, TILE)
    random_part = jnp.clip(jax.random.normal(key_list[0], shape_full, jnp.float32), -4.0, 4.0)
    spread = jax.random.uniform(key_list[1], (NBR, NBC, 4, 1, 1), jnp.float32, 0.7, 1.4)
    entries = 0.5 * random_part * spread / math.sqrt(TILE)
    identity = jnp.eye(TILE, dtype=jnp.float32)
    slot_mask = (jnp.arange(4) == 0).astype(jnp.float32)[:, None, None]
    return entries + 2.0 * slot_mask * identity


def draw_tile_codes(key, part):
    missing = jax.random.randint(jax.random.fold_in(key, 23), (NBR, NBC, 1), 0, 4, dtype=jnp.int32)
    offsets = jnp.arange(1, 4, dtype=jnp.int32)[None, None, :]
    return ((missing + offsets) % 4).astype(jnp.int32)


def draw_earlier(key, part):
    key_list = jax.random.split(jax.random.fold_in(key, 37), 2)
    shape_full = (PREV, NBR, NBC, TILE)
    random_part = jnp.clip(jax.random.normal(key_list[0], shape_full, jnp.float32), -4.0, 4.0)
    factor = jax.random.uniform(key_list[1], (1, NBR, NBC, 1), jnp.float32, 0.7, 1.4)
    row_level = jnp.arange(NBR, dtype=jnp.float32) / max(NBR - 1, 1)
    col_level = jnp.arange(NBC, dtype=jnp.float32) / max(NBC - 1, 1)
    profile = jnp.exp(math.log(3.0) * (row_level[:, None] + col_level[None, :]))
    raw = (random_part * factor * profile[None, :, :, None]).reshape(PREV, -1).T
    ortho, upper = jnp.linalg.qr(raw)
    total_cells = float(NBR * NBC * TILE)
    return (ortho.T * jnp.sqrt(total_cells)).reshape(shape_full).astype(jnp.float32)


def bell_draw(rng, dims, scale, most, held_as=jnp.bfloat16):
    array = jax.random.normal(rng, dims, jnp.float32) * scale
    return jnp.minimum(jnp.maximum(array, -most), most).astype(held_as)


def setup_inputs(seed: int = 0, part: int = 0) -> dict:
    seeds = jax.random.split(jax.random.key(seed), 7)
    part_splits = jax.random.split(jax.random.fold_in(seeds[6], part), 7)
    return {
        "tile_blocks": draw_tile_blocks(jax.random.fold_in(jax.random.fold_in(seeds[6], part), 71), part),
        "tile_codes": draw_tile_codes(jax.random.fold_in(jax.random.fold_in(seeds[6], part), 71), part),
        "shifts": jnp.clip(jax.random.uniform(part_splits[2], (BASIS,), jnp.float32, 1.2, 2.8), 1.2, 2.8),
        "shift_order": jax.random.permutation(part_splits[3], BASIS).astype(jnp.int32),
        "earlier": draw_earlier(jax.random.fold_in(jax.random.fold_in(seeds[6], part), 71), part),
        "start_weights": bell_draw(part_splits[5], (PREV,), 0.25, 1.0, jnp.float32),
    }


highest = lax.Precision.HIGHEST

def apply_operator(tile_blocks, tile_codes, vector):
    padded = jnp.pad(vector, ((1, 1), (1, 1), (0, 0)))
    beside = (padded[:-2, 1:-1], padded[2:, 1:-1], padded[1:-1, :-2], padded[1:-1, 2:])
    slots = [vector]
    for slot_index in range(3):
        code_column = tile_codes[:, :, slot_index]
        chosen = jnp.zeros_like(vector)
        for direction in range(4):
            chosen = chosen + jnp.where((code_column == direction)[:, :, None], beside[direction], jnp.zeros_like(vector))
        slots.append(chosen)
    stacked = jnp.stack(slots, axis=2)
    return jnp.einsum('rckij,rckj->rci', tile_blocks, stacked, precision=highest)

def reference(tile_blocks, tile_codes, shifts, shift_order, earlier, start_weights):
    picker = (shift_order[:, None] == jnp.arange(BASIS, dtype=jnp.int32)[None, :]).astype(shifts.dtype)
    shift_values = jnp.dot(picker, shifts, precision=highest)
    current = jnp.einsum('p,prct->rct', start_weights, earlier, precision=highest)
    columns = []
    for step_index in range(BASIS):
        current = apply_operator(tile_blocks, tile_codes, current) - shift_values[step_index] * current
        columns.append(current)
    powers = jnp.stack(columns)
    total_cells = float(NBR * NBC * TILE)
    projections = jnp.einsum('prct,srct->ps', earlier, powers, precision=highest) / total_cells
    cleaned = powers - jnp.einsum('ps,prct->srct', projections, earlier, precision=highest)
    flat = cleaned.reshape(BASIS, -1).T
    ortho, upper = jnp.linalg.qr(flat)
    signs = jnp.sign(jnp.diagonal(upper))
    upper_factor = upper * signs[:, None] / jnp.sqrt(total_cells)
    new_basis = (ortho * signs[None, :]).T.reshape(BASIS, NBR, NBC, TILE) * jnp.sqrt(total_cells)
    return (new_basis, upper_factor, projections)
```

```python
import functools

import jax
import jax.numpy as jnp
from jax import lax
from jax.experimental import pallas as pl
from jax.experimental.pallas import tpu as pltpu
from jax.sharding import PartitionSpec as P

MESH = pl.DeviceIdType.MESH
ABOVE, BELOW, LEFT, RIGHT = range(4)


def kernel(
    n_rows, n_cols,
    blocks_hbm, codes_ref, shifts_ref, order_ref, earlier_hbm, weights_ref,
    basis_ref, upper_ref, proj_ref,
    blocks, earlier, fields, chosen, halo_rows, halo_cols, edge_cols, stats, gathered, spread,
    load_sem, earlier_sem, send_sem, recv_sem, all_send, all_recv,
):
    rows, cols, slots, tile, _ = blocks.shape
    basis = basis_ref.shape[0]
    prev = earlier.shape[0]
    groups_prev = prev // basis
    peers = n_rows * n_cols
    cells = float(peers * rows * cols * tile)
    my_row, my_col = lax.axis_index("rows"), lax.axis_index("cols")
    me = my_row * n_cols + my_col

    def load(r, c):
        return pltpu.make_async_copy(
            blocks_hbm.at[r, c], blocks.at[r, c], load_sem.at[r, c]
        )

    earlier_copy = pltpu.make_async_copy(earlier_hbm, earlier, earlier_sem)
    earlier_copy.start()
    rim_rows = [0, rows - 1]
    middle = list(range(1, rows - 1))
    for r in rim_rows:
        for c in range(cols):
            load(r, c).start()
    for r in middle:
        for c in (0, cols - 1):
            load(r, c).start()
    for r in middle:
        for c in range(1, cols - 1):
            load(r, c).start()

    barrier = pltpu.get_barrier_semaphore()

    def place(index):
        return {"rows": index // n_cols, "cols": index % n_cols}

    @pl.loop(1, peers)
    def _(d):
        pl.semaphore_signal(
            barrier, inc=1, device_id=place((me + d) % peers), device_id_type=MESH
        )

    for k in range(1, basis + 1):
        fields[k] = jnp.zeros((rows, cols, tile), jnp.float32)
    stats[...] = jnp.zeros_like(stats)
    no_row = jnp.zeros((basis, cols, tile), jnp.float32)
    no_col = jnp.zeros((basis, rows, tile), jnp.float32)
    has = [my_row > 0, my_row < n_rows - 1, my_col > 0, my_col < n_cols - 1]

    @pl.when(my_row == 0)
    def _():
        halo_rows[:, 0] = no_row

    @pl.when(my_row == n_rows - 1)
    def _():
        halo_rows[:, 1] = no_row

    @pl.when(my_col == 0)
    def _():
        halo_cols[:, 0] = no_col

    @pl.when(my_col == n_cols - 1)
    def _():
        halo_cols[:, 1] = no_col

    def hop(k, direction):
        if direction == ABOVE:
            src, dst, where_to = fields.at[k, 0], halo_rows.at[k, 1], {"rows": my_row - 1}
        elif direction == BELOW:
            src, dst, where_to = fields.at[k, rows - 1], halo_rows.at[k, 0], {"rows": my_row + 1}
        elif direction == LEFT:
            src, dst, where_to = edge_cols.at[k, 0], halo_cols.at[k, 1], {"cols": my_col - 1}
        else:
            src, dst, where_to = edge_cols.at[k, 1], halo_cols.at[k, 0], {"cols": my_col + 1}
        return pltpu.make_async_remote_copy(
            src_ref=src,
            dst_ref=dst,
            send_sem=send_sem.at[k, direction],
            recv_sem=recv_sem.at[k, direction ^ 1],
            device_id=where_to,
            device_id_type=MESH,
        )

    def arrival(k, direction):
        if direction in (ABOVE, BELOW):
            dst = halo_rows.at[k, direction]
        else:
            dst = halo_cols.at[k, direction - 2]
        return pltpu.make_async_copy(dst, dst, recv_sem.at[k, direction])

    def send(k, directions):
        for direction in directions:
            @pl.when(has[direction])
            def _(direction=direction):
                hop(k, direction).start()

    def receive(k):
        for direction in range(4):
            @pl.when(has[direction])
            def _(direction=direction):
                arrival(k, direction).wait()

    codes = codes_ref[...]
    masks = [
        [
            jnp.broadcast_to(codes[r, :, s : s + 1], (cols, tile))
            for r in range(rows)
        ]
        for s in range(slots - 1)
    ]
    sublane = lax.broadcasted_iota(jnp.int32, (cols, tile), 0)
    lane = lax.broadcasted_iota(jnp.int32, (basis, tile), 1)

    def choose(k):
        for r in range(rows):
            here = fields[k, r]
            above = fields[k, r - 1] if r > 0 else halo_rows[k, 0]
            below = fields[k, r + 1] if r < rows - 1 else halo_rows[k, 1]
            left = jnp.where(sublane == 0, halo_cols[k, 0, r : r + 1], pltpu.roll(here, 1, 0))
            right = jnp.where(
                sublane == cols - 1, halo_cols[k, 1, r : r + 1], pltpu.roll(here, cols - 1, 0)
            )
            chosen[0, r] = here
            for s in range(slots - 1):
                code = masks[s][r]
                chosen[s + 1, r] = jnp.where(
                    code < 2,
                    jnp.where(code == 0, above, below),
                    jnp.where(code == 2, left, right),
                )

    def cell(k, shift, r, c):
        total = blocks[r, c, 0] * chosen[0, r, c : c + 1]
        for s in range(1, slots):
            total = total + blocks[r, c, s] * chosen[s, r, c : c + 1]
        product = jnp.sum(total.T, axis=0, keepdims=True)
        fields[k + 1, r, c : c + 1] = product - shift * chosen[0, r, c : c + 1]

    def row_of_cells(k, shift, r, columns, first):
        for c in columns:
            if first:
                load(r, c).wait()
            cell(k, shift, r, c)

    def inner(k):
        field = fields[k + 1]
        merged = stats[...]
        for g in range(groups_prev + 1):
            if g < groups_prev:
                other = earlier[g * basis : (g + 1) * basis]
            else:
                other = fields[1 : basis + 1]
            pair = jnp.sum(jnp.sum(other * field[None], axis=1), axis=1)
            value = jnp.sum(pair, axis=1, keepdims=True)
            merged = jnp.where(lane == g * basis + k, value, merged)
        stats[...] = merged

    def step(k, first):
        shift = shifts_ref[order_ref[k]]
        receive(k)
        choose(k)

        @pl.loop(0, 2)
        def _(side):
            row_of_cells(k, shift, side * (rows - 1), range(cols), first)

        last = isinstance(k, int) and k == basis - 1
        if not last:
            send(k + 1, (ABOVE, BELOW))

        @pl.loop(1, rows - 1)
        def _(r):
            row_of_cells(k, shift, r, (0, cols - 1), first)

        if not last:
            for r in range(rows):
                edge_cols[k + 1, 0, r : r + 1] = fields[k + 1, r, 0:1]
                edge_cols[k + 1, 1, r : r + 1] = fields[k + 1, r, cols - 1 : cols]
            send(k + 1, (LEFT, RIGHT))

        @pl.loop(1, rows - 1)
        def _(r):
            row_of_cells(k, shift, r, range(1, cols - 1), first)

        inner(k)

    earlier_copy.wait()
    start = weights_ref[0] * earlier[0]
    for p in range(1, prev):
        start = start + weights_ref[p] * earlier[p]
    fields[0] = start
    for r in range(rows):
        edge_cols[0, 0, r : r + 1] = fields[0, r, 0:1]
        edge_cols[0, 1, r : r + 1] = fields[0, r, cols - 1 : cols]
    pl.semaphore_wait(barrier, peers - 1)
    send(0, (ABOVE, BELOW, LEFT, RIGHT))
    step(0, True)

    @pl.loop(1, basis - 1)
    def _(k):
        step(k, False)

    step(basis - 1, False)

    def deliver(d):
        return pltpu.make_async_remote_copy(
            src_ref=stats,
            dst_ref=gathered.at[me],
            send_sem=all_send.at[d],
            recv_sem=all_recv.at[me],
            device_id=place((me + d) % peers),
            device_id_type=MESH,
        )

    @pl.loop(1, peers)
    def _(d):
        deliver(d).start()

    gathered[me] = stats[...]

    @pl.loop(1, peers)
    def _(d):
        source = (me + d) % peers
        pltpu.make_async_copy(
            gathered.at[source], gathered.at[source], all_recv.at[source]
        ).wait()

    total = jnp.sum(gathered[...], axis=0) * (1.0 / cells)
    proj = []
    for i in range((groups_prev + 1) * basis):
        column = jnp.broadcast_to(total[:, i : i + 1], (basis, tile))
        spread[i] = column
        proj.append(column)
    for g in range(groups_prev):
        proj_ref[g * basis : (g + 1) * basis, :] = total[:, g * basis : (g + 1) * basis]

    cleaned = []
    for k in range(basis):
        value = fields[k + 1]
        for p in range(prev):
            g, q = p // basis, p % basis
            value = value - spread[g * basis + k, q : q + 1][None] * earlier[p]
        basis_ref[k] = value

    gram = {}
    for j in range(basis):
        for k in range(j, basis):
            removed = proj[j] * proj[k]
            for g in range(1, groups_prev):
                removed = removed + proj[g * basis + j] * proj[g * basis + k]
            gram[j, k] = spread[groups_prev * basis + k, j : j + 1] - jnp.sum(
                removed, axis=0, keepdims=True
            )
    lower, inverse = {}, []
    for j in range(basis):
        root = jnp.sqrt(gram[j, j])
        inverse.append(1.0 / root)
        lower[j, j] = root
        for k in range(j + 1, basis):
            lower[k, j] = gram[j, k] * inverse[j]
        for k in range(j + 1, basis):
            for m in range(k, basis):
                gram[k, m] = gram[k, m] - lower[k, j] * lower[m, j]

    row_index = lax.broadcasted_iota(jnp.int32, (basis, tile), 0)
    upper = jnp.zeros((basis, tile), jnp.float32)
    for j in range(basis):
        line = jnp.zeros((1, tile), jnp.float32)
        for k in range(j, basis):
            line = jnp.where(lane[0:1] == k, lower[k, j], line)
        upper = jnp.where(row_index == j, line, upper)
    upper_ref[...] = upper[:, :basis]

    for r in range(rows):
        done = []
        for k in range(basis):
            value = basis_ref[k, r]
            for j in range(k):
                value = value - lower[k, j] * done[j]
            value = value * inverse[k]
            done.append(value)
            basis_ref[k, r] = value

    @pl.loop(0, basis)
    def _(k):
        for direction in range(4):
            @pl.when(has[direction])
            def _(direction=direction):
                hop(k, direction).wait_send()

    @pl.loop(1, peers)
    def _(d):
        deliver(d).wait_send()


def shards(n_rows, n_cols, tile_blocks, tile_codes, shifts, shift_order, earlier, start_weights):
    rows, cols, slots, tile, _ = tile_blocks.shape
    basis, prev = shifts.shape[0], earlier.shape[0]
    peers = n_rows * n_cols
    vmem = pl.BlockSpec(memory_space=pltpu.VMEM)
    smem = pl.BlockSpec(memory_space=pltpu.SMEM)
    anywhere = pl.BlockSpec(memory_space=pl.ANY)
    f32 = jnp.float32
    return pl.pallas_call(
        functools.partial(kernel, n_rows, n_cols),
        out_shape=(
            jax.ShapeDtypeStruct((basis, rows, cols, tile), f32),
            jax.ShapeDtypeStruct((basis, basis), f32),
            jax.ShapeDtypeStruct((prev, basis), f32),
        ),
        in_specs=[anywhere, vmem, smem, smem, anywhere, smem],
        out_specs=(vmem, vmem, vmem),
        scratch_shapes=[
            pltpu.VMEM(tile_blocks.shape, f32),
            pltpu.VMEM(earlier.shape, f32),
            pltpu.VMEM((basis + 1, rows, cols, tile), f32),
            pltpu.VMEM((slots, rows, cols, tile), f32),
            pltpu.VMEM((basis, 2, cols, tile), f32),
            pltpu.VMEM((basis, 2, rows, tile), f32),
            pltpu.VMEM((basis, 2, rows, tile), f32),
            pltpu.VMEM((basis, tile), f32),
            pltpu.VMEM((peers, basis, tile), f32),
            pltpu.VMEM(((prev // basis + 1) * basis, basis, tile), f32),
            pltpu.SemaphoreType.DMA((rows, cols)),
            pltpu.SemaphoreType.DMA,
            pltpu.SemaphoreType.DMA((basis, 4)),
            pltpu.SemaphoreType.DMA((basis, 4)),
            pltpu.SemaphoreType.DMA((peers,)),
            pltpu.SemaphoreType.DMA((peers,)),
        ],
        compiler_params=pltpu.CompilerParams(
            collective_id=0, has_side_effects=True, vmem_limit_bytes=48 * 1024 * 1024
        ),
        name="sstep",
    )(tile_blocks, tile_codes, shifts, shift_order, earlier, start_weights)


def solution(mesh):
    in_specs = (
        P(("groups", "rows"), "cols", None, None, None),
        P(("groups", "rows"), "cols", None),
        P("groups"),
        P("groups"),
        P(None, ("groups", "rows"), "cols", None),
        P("groups"),
    )
    out_specs = (P(None, ("groups", "rows"), "cols", None), P("groups", None), P("groups", None))
    body = functools.partial(shards, mesh.shape["rows"], mesh.shape["cols"])
    return jax.shard_map(body, mesh=mesh, in_specs=in_specs, out_specs=out_specs, check_vma=False)
```

```python
import functools

import jax
import jax.numpy as jnp
from jax import lax
from jax.experimental import pallas as pl
from jax.experimental.pallas import tpu as pltpu
from jax.sharding import PartitionSpec as P

MESH = pl.DeviceIdType.MESH
ABOVE, BELOW, LEFT, RIGHT = range(4)


def kernel(
    n_rows, n_cols,
    blocks_hbm, codes_hbm, shifts_hbm, order_hbm, earlier_hbm, weights_hbm,
    basis_ref, upper_ref, proj_ref,
    blocks, earlier, codes_ref, shifts_ref, order_ref, weights_ref,
    fields, chosen, halo_rows, halo_cols, edge_cols, rim_rows, rim_cols,
    code_table, stats, gathered, spread,
    load_sem, small_sem, send_sem, recv_sem, all_send, all_recv,
):
    rows, cols, slots, tile, _ = blocks.shape
    basis = basis_ref.shape[0]
    prev = earlier.shape[0]
    groups_prev = prev // basis
    peers = n_rows * n_cols
    cells = float(peers * rows * cols * tile)
    my_row, my_col = lax.axis_index("rows"), lax.axis_index("cols")
    me = my_row * n_cols + my_col

    def load(r, c):
        return pltpu.make_async_copy(
            blocks_hbm.at[r, c], blocks.at[r, c], load_sem.at[r, c]
        )

    small = [
        pltpu.make_async_copy(src, dst, small_sem.at[i])
        for i, (src, dst) in enumerate(
            [
                (weights_hbm, weights_ref),
                (earlier_hbm, earlier),
                (codes_hbm, codes_ref),
                (shifts_hbm, shifts_ref),
                (order_hbm, order_ref),
            ]
        )
    ]
    for copy in small:
        copy.start()
    for r in range(rows):
        for c in range(cols):
            load(r, c).start()

    barrier = pltpu.get_barrier_semaphore()

    def place(index):
        return {"rows": index // n_cols, "cols": index % n_cols}

    @pl.loop(1, peers)
    def _(d):
        pl.semaphore_signal(
            barrier, inc=1, device_id=place((me + d) % peers), device_id_type=MESH
        )

    for k in range(1, basis + 1):
        fields[k] = jnp.zeros((rows, cols, tile), jnp.float32)
    stats[...] = jnp.zeros_like(stats)
    no_row = jnp.zeros((basis, cols, tile), jnp.float32)
    no_col = jnp.zeros((basis, rows, tile), jnp.float32)
    has = [my_row > 0, my_row < n_rows - 1, my_col > 0, my_col < n_cols - 1]

    @pl.when(my_row == 0)
    def _():
        halo_rows[:, 0] = no_row

    @pl.when(my_row == n_rows - 1)
    def _():
        halo_rows[:, 1] = no_row

    @pl.when(my_col == 0)
    def _():
        halo_cols[:, 0] = no_col

    @pl.when(my_col == n_cols - 1)
    def _():
        halo_cols[:, 1] = no_col

    def hop(k, direction):
        if direction == ABOVE:
            src, dst, where_to = fields.at[k, 0], halo_rows.at[k, 1], {"rows": my_row - 1}
        elif direction == BELOW:
            src, dst, where_to = fields.at[k, rows - 1], halo_rows.at[k, 0], {"rows": my_row + 1}
        elif direction == LEFT:
            src, dst, where_to = edge_cols.at[k, 0], halo_cols.at[k, 1], {"cols": my_col - 1}
        else:
            src, dst, where_to = edge_cols.at[k, 1], halo_cols.at[k, 0], {"cols": my_col + 1}
        return pltpu.make_async_remote_copy(
            src_ref=src,
            dst_ref=dst,
            send_sem=send_sem.at[k, direction],
            recv_sem=recv_sem.at[k, direction ^ 1],
            device_id=where_to,
            device_id_type=MESH,
        )

    def arrival(k, direction):
        if direction in (ABOVE, BELOW):
            dst = halo_rows.at[k, direction]
        else:
            dst = halo_cols.at[k, direction - 2]
        return pltpu.make_async_copy(dst, dst, recv_sem.at[k, direction])

    def send(k, directions):
        for direction in directions:
            @pl.when(has[direction])
            def _(direction=direction):
                hop(k, direction).start()

    def receive(k):
        for direction in range(4):
            @pl.when(has[direction])
            def _(direction=direction):
                arrival(k, direction).wait()

    sublane = lax.broadcasted_iota(jnp.int32, (cols, tile), 0)
    lane = lax.broadcasted_iota(jnp.int32, (basis, tile), 1)
    diagonal = lax.broadcasted_iota(jnp.int32, (cols, cols), 0) == lax.broadcasted_iota(
        jnp.int32, (cols, cols), 1
    )

    def code_columns():
        codes = codes_ref[...].astype(jnp.float32)
        masks = []
        for s in range(slots - 1):
            masks.append([])
            for r in range(rows):
                line = jnp.broadcast_to(codes[s, r : r + 1], (cols, cols))
                column = jnp.sum(jnp.where(diagonal, line, 0.0), axis=1, keepdims=True)
                masks[s].append(jnp.broadcast_to(column, (cols, tile)))
        return masks

    def choose(k):
        none = jnp.zeros((cols, tile), jnp.float32)
        for r in range(rows):
            here = fields[k, r]
            above = fields[k, r - 1] if r > 0 else none
            below = fields[k, r + 1] if r < rows - 1 else none
            left = jnp.where(sublane == 0, 0.0, pltpu.roll(here, 1, 0))
            right = jnp.where(sublane == cols - 1, 0.0, pltpu.roll(here, cols - 1, 0))
            chosen[0, r] = here
            for s in range(slots - 1):
                code = code_table[s, r]
                chosen[s + 1, r] = jnp.where(
                    code < 1.5,
                    jnp.where(code < 0.5, above, below),
                    jnp.where(code < 2.5, left, right),
                )

    def inside(k, first):
        shift = shifts_ref[order_ref[k]]
        choose(k)

        @pl.loop(0, rows)
        def _(r):
            if first:
                for c in range(cols):
                    load(r, c).wait()
            for c in range(cols):
                total = blocks[r, c, 0] * chosen[0, r, c : c + 1]
                for s in range(1, slots):
                    total = total + blocks[r, c, s] * chosen[s, r, c : c + 1]
                product = jnp.sum(total.T, axis=0, keepdims=True)
                fields[k + 1, r, c : c + 1] = product - shift * chosen[0, r, c : c + 1]

    def pick(r, c, direction):
        total = jnp.zeros((tile, tile), jnp.float32)
        for s in range(slots - 1):
            code = code_table[s, r, c : c + 1]
            total = jnp.where(code == float(direction), blocks[r, c, s + 1], total)
        return total

    def gather_rim():
        for side in range(2):
            @pl.loop(0, cols)
            def _(c, side=side):
                total = jnp.zeros((tile, tile), jnp.float32)
                for s in range(slots - 1):
                    code = code_table[s, side * (rows - 1), pl.ds(c, 1)]
                    total = jnp.where(
                        code == float(side), blocks[side * (rows - 1), c, s + 1], total
                    )
                rim_rows[side, c] = total

            @pl.loop(0, rows)
            def _(r, side=side):
                rim_cols[side, r] = pick(r, side * (cols - 1), side + LEFT)

    def rim(k):
        for r in range(rows):
            for c in range(cols):
                parts = []
                for side in range(2):
                    if r == side * (rows - 1):
                        parts.append(rim_rows[side, c] * halo_rows[k, side, c : c + 1])
                    if c == side * (cols - 1):
                        parts.append(rim_cols[side, r] * halo_cols[k, side, r : r + 1])
                if parts:
                    product = jnp.sum(sum(parts[1:], parts[0]).T, axis=0, keepdims=True)
                    fields[k + 1, r, c : c + 1] += product

    def edges(k):
        for r in range(rows):
            edge_cols[k, 0, r : r + 1] = fields[k, r, 0:1]
            edge_cols[k, 1, r : r + 1] = fields[k, r, cols - 1 : cols]

    def inner(k):
        field = fields[k + 1]
        merged = stats[...]
        for g in range(groups_prev + 1):
            if g < groups_prev:
                other = earlier[g * basis : (g + 1) * basis]
            else:
                other = fields[1 : basis + 1]
            pair = jnp.sum(jnp.sum(other * field[None], axis=1), axis=1)
            value = jnp.sum(pair, axis=1, keepdims=True)
            merged = jnp.where(lane == g * basis + k, value, merged)
        stats[...] = merged

    small[0].wait()
    small[1].wait()
    start = weights_ref[0] * earlier[0]
    for p in range(1, prev):
        start = start + weights_ref[p] * earlier[p]
    fields[0] = start
    edges(0)
    for copy in small[2:]:
        copy.wait()
    for s, lines in enumerate(code_columns()):
        for r, line in enumerate(lines):
            code_table[s, r] = line
    pl.semaphore_wait(barrier, peers - 1)
    send(0, (ABOVE, BELOW, LEFT, RIGHT))
    inside(0, True)
    gather_rim()

    @pl.loop(0, basis - 1)
    def _(k):
        receive(k)
        rim(k)
        edges(k + 1)
        send(k + 1, (ABOVE, BELOW, LEFT, RIGHT))
        inside(k + 1, False)
        inner(k)

    receive(basis - 1)
    rim(basis - 1)
    inner(basis - 1)

    def deliver(d):
        return pltpu.make_async_remote_copy(
            src_ref=stats,
            dst_ref=gathered.at[me],
            send_sem=all_send.at[d],
            recv_sem=all_recv.at[me],
            device_id=place((me + d) % peers),
            device_id_type=MESH,
        )

    @pl.loop(1, peers)
    def _(d):
        deliver(d).start()

    gathered[me] = stats[...]

    @pl.loop(1, peers)
    def _(d):
        source = (me + d) % peers
        pltpu.make_async_copy(
            gathered.at[source], gathered.at[source], all_recv.at[source]
        ).wait()

    total = jnp.sum(gathered[...], axis=0) * (1.0 / cells)
    proj = []
    for i in range((groups_prev + 1) * basis):
        column = jnp.broadcast_to(total[:, i : i + 1], (basis, tile))
        spread[i] = column
        proj.append(column)
    turned = total.T
    for g in range(groups_prev):
        proj_ref[:, g * basis : (g + 1) * basis] = turned[g * basis : (g + 1) * basis, :]

    cleaned = []
    for k in range(basis):
        value = fields[k + 1]
        for p in range(prev):
            g, q = p // basis, p % basis
            value = value - spread[g * basis + k, q : q + 1][None] * earlier[p]
        basis_ref[k] = value

    gram = {}
    for j in range(basis):
        for k in range(j, basis):
            removed = proj[j] * proj[k]
            for g in range(1, groups_prev):
                removed = removed + proj[g * basis + j] * proj[g * basis + k]
            gram[j, k] = spread[groups_prev * basis + k, j : j + 1] - jnp.sum(
                removed, axis=0, keepdims=True
            )
    lower, inverse = {}, []
    for j in range(basis):
        root = jnp.sqrt(gram[j, j])
        inverse.append(1.0 / root)
        lower[j, j] = root
        for k in range(j + 1, basis):
            lower[k, j] = gram[j, k] * inverse[j]
        for k in range(j + 1, basis):
            for m in range(k, basis):
                gram[k, m] = gram[k, m] - lower[k, j] * lower[m, j]

    row_index = lax.broadcasted_iota(jnp.int32, (basis, tile), 0)
    upper = jnp.zeros((basis, tile), jnp.float32)
    for j in range(basis):
        line = jnp.zeros((1, tile), jnp.float32)
        for k in range(j, basis):
            line = jnp.where(lane[0:1] == k, lower[k, j], line)
        upper = jnp.where(row_index == j, line, upper)
    upper_ref[...] = upper[:, :basis]

    for r in range(rows):
        done = []
        for k in range(basis):
            value = basis_ref[k, r]
            for j in range(k):
                value = value - lower[k, j] * done[j]
            value = value * inverse[k]
            done.append(value)
            basis_ref[k, r] = value

    @pl.loop(0, basis)
    def _(k):
        for direction in range(4):
            @pl.when(has[direction])
            def _(direction=direction):
                hop(k, direction).wait_send()

    @pl.loop(1, peers)
    def _(d):
        deliver(d).wait_send()


def shards(n_rows, n_cols, tile_blocks, tile_codes, shifts, shift_order, earlier, start_weights):
    rows, cols, slots, tile, _ = tile_blocks.shape
    basis, prev = shifts.shape[0], earlier.shape[0]
    peers = n_rows * n_cols
    vmem = pl.BlockSpec(memory_space=pltpu.VMEM)
    hbm = pl.BlockSpec(memory_space=pltpu.HBM)
    codes = jnp.transpose(tile_codes, (2, 0, 1))
    f32 = jnp.float32
    basis_out, upper, proj = pl.pallas_call(
        functools.partial(kernel, n_rows, n_cols),
        out_shape=(
            jax.ShapeDtypeStruct((basis, rows, cols, tile), f32),
            jax.ShapeDtypeStruct((basis, basis), f32),
            jax.ShapeDtypeStruct((basis, prev), f32),
        ),
        in_specs=[hbm] * 6,
        out_specs=(vmem, vmem, vmem),
        scratch_shapes=[
            pltpu.VMEM(tile_blocks.shape, f32),
            pltpu.VMEM(earlier.shape, f32),
            pltpu.VMEM(codes.shape, jnp.int32),
            pltpu.SMEM(shifts.shape, f32),
            pltpu.SMEM(shift_order.shape, jnp.int32),
            pltpu.SMEM(start_weights.shape, f32),
            pltpu.VMEM((basis + 1, rows, cols, tile), f32),
            pltpu.VMEM((slots, rows, cols, tile), f32),
            pltpu.VMEM((basis, 2, cols, tile), f32),
            pltpu.VMEM((basis, 2, rows, tile), f32),
            pltpu.VMEM((basis, 2, rows, tile), f32),
            pltpu.VMEM((2, cols, tile, tile), f32),
            pltpu.VMEM((2, rows, tile, tile), f32),
            pltpu.VMEM((slots - 1, rows, cols, tile), f32),
            pltpu.VMEM((basis, tile), f32),
            pltpu.VMEM((peers, basis, tile), f32),
            pltpu.VMEM(((prev // basis + 1) * basis, basis, tile), f32),
            pltpu.SemaphoreType.DMA((rows, cols)),
            pltpu.SemaphoreType.DMA((5,)),
            pltpu.SemaphoreType.DMA((basis, 4)),
            pltpu.SemaphoreType.DMA((basis, 4)),
            pltpu.SemaphoreType.DMA((peers,)),
            pltpu.SemaphoreType.DMA((peers,)),
        ],
        compiler_params=pltpu.CompilerParams(
            collective_id=0, has_side_effects=True, vmem_limit_bytes=67_043_328
        ),
        name="sstep",
    )(tile_blocks, codes, shifts, shift_order, earlier, start_weights)
    return basis_out, upper, proj.T


def solution(mesh):
    in_specs = (
        P(("groups", "rows"), "cols", None, None, None),
        P(("groups", "rows"), "cols", None),
        P("groups"),
        P("groups"),
        P(None, ("groups", "rows"), "cols", None),
        P("groups"),
    )
    out_specs = (P(None, ("groups", "rows"), "cols", None), P("groups", None), P("groups", None))
    body = functools.partial(shards, mesh.shape["rows"], mesh.shape["cols"])
    return jax.shard_map(body, mesh=mesh, in_specs=in_specs, out_specs=out_specs, check_vma=False)
```
